32 devices in a mesh: row: 4 (over z), col: 8 (over y, x, core).
Axes of the slice: x: 2, y: 2, z: 4, core: 2. Of those that a mesh axis runs over, the one named last changes fastest.
Arguments:
- air_flux: bfloat16 [4, 4096, 16, 128], P(None, ('row', 'col')), may hold values from -1 to 3
- air_area: float32 [4096, 128], P(('row', 'col')), may hold values from 0.2 to 2
- sea_area: float32 [4096, 128], P(('row', 'col')), may hold values from 0.2 to 2
- wet_mask: int32 [4096], P(('row', 'col')), may hold values 0 or 1
- intersection_tiles: bfloat16 [32, 128, 128], replicated, may hold values from -0.125 to 0.125
- send_block: int32 [32, 256], P(('row', 'col')), may hold values from 0 to 127
- target_slot: int32 [4096, 16], P(('row', 'col')), may hold values from 0 to 255
- target_tile: int32 [4096, 16], P(('row', 'col')), may hold values from 0 to 31, as said below
Outputs:
- sea_flux: float32 [4096, 16, 128], P(('row', 'col'))
The draws below stay inside these ranges and needn't reach their ends.
Inputs may be any that keep to these rules, and one draw needn't show every extreme that they name: `target_tile`: the 16 entries of a row are distinct.
All inputs are finite; a program needn't handle non-finite values. No bound on the sum of `wet_mask` on one device may be relied on, other than what follows from the above.
Results may differ from the reference program's by a relative error of at most 0.0003.
The reference program's roundings to bfloat16 on the way (of `sent_flux`) count: a program that leaves them out, or rounds other values in their place, can miss the bound.
Values may be sent and summed in bfloat16 or wider, within the bound.
No kernel may reach another device: no remote copies, remote signals or barrier semaphores. Data moves between devices by JAX's collectives and lax.ppermute only.
A program may use at most 128 MiB of HBM per device.

```python
import math
import jax
import jax.numpy as jnp
from jax import lax

F = 16
CELLS = 128
K = 16
NTILES = 32
NSTEPS = 4
SB_DEV = 128
CAP = 32
NBLK = 4096
N_ROW = 4
N_COL = 8


def draw_target_tile(key, part):
    scores = jax.random.randint(key, (NBLK, NTILES), 0, 1 << 20) * NTILES + jnp.arange(NTILES, dtype=jnp.int32)[None, :]
    order = jnp.argsort(scores, axis=1, stable=True)
    return order[:, :K].astype(jnp.int32)


def set_ends(result, rng, low, top_value):
    place = [jax.random.randint(jax.random.fold_in(rng, axis), (), 0, length) for axis, length in enumerate(result.shape)]
    main_axis = result.shape.index(max(result.shape))
    next_to = place[:main_axis] + [(place[main_axis] + 1) % result.shape[main_axis]] + place[main_axis + 1:]
    return result.at[tuple(place)].set(low).at[tuple(next_to)].set(top_value)


def level_of(stream_key, extent, shards, least, largest):
    def one(axis_at, shards_of):
        draws = jax.random.uniform(jax.random.fold_in(jax.random.fold_in(stream_key, 6), axis_at), (shards_of,), jnp.float32, least / len(shards), largest / len(shards))
        return jnp.repeat(jnp.exp(draws), extent[axis_at] // shards_of).reshape((-1,) + (1,) * (len(extent) - axis_at - 1))

    level = one(*shards[0])
    for cut in shards[1:]:
        level = level * one(*cut)
    return level


def scatter_about(key, extent, scale, limit, held_as=jnp.bfloat16):
    drawn = jax.random.normal(key, extent, jnp.float32) * scale
    return jnp.minimum(jnp.maximum(drawn, -limit), limit).astype(held_as)


def setup_inputs(seed: int = 0) -> dict:
    keys = jax.random.split(jax.random.key(seed), 9)
    air_flux = jnp.clip(-1.0 + 4.0 * jax.random.uniform(keys[0], (NSTEPS, NBLK, F, CELLS), jnp.float32) ** level_of(keys[0], (NSTEPS, NBLK, F, CELLS), ((1, 32),), -0.2, 0.2), -1.0, 3.0).astype(jnp.bfloat16)
    air_area = jnp.clip(jnp.exp(math.log(2.0) - 2.3025851 * jax.random.uniform(keys[1], (NBLK, CELLS), jnp.float32) ** level_of(keys[1], (NBLK, CELLS), ((0, 32),), -0.2, 0.2)), 0.2, 2.0)
    sea_area = jnp.clip(jnp.exp(math.log(2.0) - 2.3025851 * jax.random.uniform(keys[2], (NBLK, CELLS), jnp.float32) ** level_of(keys[2], (NBLK, CELLS), ((0, 32),), -0.2, 0.2)), 0.2, 2.0)
    wet_mask = set_ends((jax.random.randint(keys[3], (NBLK,), 0, 4) < 3).astype(jnp.int32), jax.random.fold_in(keys[3], 1), 0, 1)
    intersection_tiles = scatter_about(keys[4], (NTILES, CELLS, CELLS), (K * CELLS) ** -0.5, 0.125)
    send_block = set_ends(jax.random.randint(keys[5], (N_ROW * N_COL, N_COL * CAP), 0, SB_DEV), jax.random.fold_in(keys[5], 1), 0, SB_DEV - 1).astype(jnp.int32)
    target_slot = set_ends(jax.random.randint(keys[6], (NBLK, K), 0, N_COL * CAP), jax.random.fold_in(keys[6], 1), 0, (N_COL * CAP) - 1).astype(jnp.int32)
    target_tile = draw_target_tile(jax.random.fold_in(keys[8], 71), 0)
    return {"air_flux": air_flux, "air_area": air_area, "sea_area": sea_area, "wet_mask": wet_mask, "intersection_tiles": intersection_tiles, "send_block": send_block, "target_slot": target_slot, "target_tile": target_tile}


def reference(air_flux, air_area, sea_area, wet_mask, intersection_tiles, send_block, target_slot, target_tile):
    mean_flux = jnp.sum(air_flux, axis=0, dtype=jnp.float32) / NSTEPS
    sent_flux = mean_flux.astype(jnp.bfloat16)
    air_total = jnp.sum(mean_flux * air_area[:, None, :], axis=(0, 2))
    capacity = send_block.shape[1] // N_COL

    def one_device(device):
        band_row = device // N_COL
        column = device % N_COL
        slot_ids = lax.dynamic_slice_in_dim(target_slot, (device * SB_DEV).astype(jnp.int32), SB_DEV, 0)
        tile_ids = lax.dynamic_slice_in_dim(target_tile, (device * SB_DEV).astype(jnp.int32), SB_DEV, 0)
        sender = band_row * N_COL + slot_ids // capacity
        local_block = send_block[sender, column * capacity + slot_ids % capacity]
        source = (sender * SB_DEV + local_block).astype(jnp.int32)
        summed = jnp.zeros((SB_DEV, F, CELLS), jnp.float32)
        for intersection in range(K):
            chosen = sent_flux[source[:, intersection]].astype(jnp.float32)
            weights = intersection_tiles[tile_ids[:, intersection]].astype(jnp.float32)
            summed = summed + jnp.einsum("tfc,tcd->tfd", chosen, weights, precision=lax.Precision.HIGHEST)
        return summed

    raw_flux = lax.map(one_device, jnp.arange(N_ROW * N_COL, dtype=jnp.int32)).reshape(-1, F, CELLS)
    wet_area = wet_mask.astype(jnp.float32)[:, None] * sea_area
    sea_total = jnp.sum(raw_flux * wet_area[:, None, :], axis=(0, 2))
    wet_total = jnp.maximum(jnp.sum(wet_area), 1.0)
    shift = (air_total - sea_total) / wet_total
    return wet_mask.astype(jnp.float32)[:, None, None] * (raw_flux + shift[None, :, None])
```

```python
import functools
import jax
import jax.numpy as jnp
from jax import lax
from jax.experimental import pallas as pl
from jax.experimental.pallas import tpu as pltpu
from jax.sharding import PartitionSpec as P


VMEM = pltpu.VMEM
SMEM = pltpu.SMEM


def whole(space=VMEM):
    return pl.BlockSpec(memory_space=space)


def peers_of(columns):
    order = [peer for peer in (6, 7, 2, 3, 4, 5, 1) if peer < columns]
    return order + [peer for peer in range(8, columns)]


def piece_order(columns):
    return [0] + peers_of(columns)


def pick_kernel(send_ref, flux_ref, *refs, order, capacity, axis):
    *out_refs, mean_ref = refs
    steps, group = flux_ref.shape[:2]
    step = pl.program_id(0)
    total = flux_ref[0].astype(jnp.float32)
    for index in range(1, steps):
        total += flux_ref[index].astype(jnp.float32)
    mean_ref[pl.ds(step * group, group)] = (total * (1.0 / steps)).astype(mean_ref.dtype)

    @pl.when(step == pl.num_programs(0) - 1)
    def _():
        me = lax.axis_index(axis) if len(order) > 1 else 0
        for out_ref, offset in zip(out_refs, order):
            base = (me ^ offset) * capacity
            for slot in range(out_ref.shape[0]):
                out_ref[slot] = mean_ref[send_ref[base + slot]]


def pick(send_block, air_flux, order, axis, groups=4):
    steps, blocks, fields, cells = air_flux.shape
    slots = send_block.shape[0]
    capacity = slots // len(order)
    out = jax.ShapeDtypeStruct((capacity, fields, cells), air_flux.dtype)
    return pl.pallas_call(
        functools.partial(pick_kernel, order=order, capacity=capacity, axis=axis),
        grid=(groups,),
        out_shape=[out] * len(order),
        in_specs=[
            whole(SMEM),
            pl.BlockSpec((steps, blocks // groups, fields, cells), lambda i: (0, i, 0, 0)),
        ],
        out_specs=[pl.BlockSpec((capacity, fields, cells), lambda i: (0, 0, 0))] * len(order),
        scratch_shapes=[VMEM((blocks, fields, cells), air_flux.dtype)],
        name="pick",
    )(send_block, air_flux)


def split3(value):
    high = value.astype(jnp.bfloat16)
    rest = value - high.astype(jnp.float32)
    middle = rest.astype(jnp.bfloat16)
    low = (rest - middle.astype(jnp.float32)).astype(jnp.bfloat16)
    return high, middle, low


def lanes_of(column):
    rows, lanes = column.shape
    total = jnp.sum(column, axis=1, keepdims=True)
    on = lax.broadcasted_iota(jnp.int32, (rows, lanes), 0) == lax.broadcasted_iota(
        jnp.int32, (rows, lanes), 1
    )
    return jnp.sum(jnp.where(on, total, 0.0), axis=0, keepdims=True)


def prepare_kernel(flux_ref, area_ref, sea_ref, wet_ref, where_ref, tiles_ref, sums_ref, weight_ref, air_ref):
    steps, group, fields, cells = flux_ref.shape
    step = pl.program_id(0)

    @pl.when(step == 0)
    def _():
        air_ref[...] = jnp.zeros_like(air_ref)

    total = flux_ref[0].astype(jnp.float32)
    for index in range(1, steps):
        total += flux_ref[index].astype(jnp.float32)
    air_ref[...] += jnp.sum((total * (1.0 / steps)) * area_ref[...][:, None, :], axis=0)

    @pl.when(step == pl.num_programs(0) - 1)
    def _():
        wet_area = wet_ref[...] * sea_ref[...]
        wet_row = jnp.sum(jnp.sum(wet_area, axis=0, keepdims=True), axis=1, keepdims=True)
        lane = lax.broadcasted_iota(jnp.int32, (1, cells), 1)
        sums_ref[...] = lanes_of(air_ref[...]) + jnp.where(lane == fields, wet_row, 0.0)

        parts = jnp.concatenate(split3(wet_area), axis=0)
        targets = wet_area.shape[0]
        slots = weight_ref.shape[0]
        tiles = where_ref.shape[0]
        slot = lax.broadcasted_iota(jnp.int32, (slots, targets), 0)

        weight_ref[...] = jnp.zeros_like(weight_ref)

        def pair(index, carry):
            hits, values = [], []
            for half in range(2):
                tile = index * 2 + half
                spread = lax.dot_general(
                    parts,
                    tiles_ref[tile],
                    (((1,), (1,)), ((), ())),
                    preferred_element_type=jnp.float32,
                )
                spread = spread[:targets] + spread[targets : 2 * targets] + spread[2 * targets :]
                values.append(jnp.concatenate(split3(spread), axis=1))
                hit = slot == where_ref[pl.ds(tile, 1), :]
                hits.append(jnp.where(hit, 1.0, 0.0).astype(jnp.bfloat16))
            found = jnp.dot(
                jnp.concatenate(hits, axis=1),
                jnp.concatenate(values, axis=0),
                preferred_element_type=jnp.float32,
            )
            weight_ref[...] += found[:, :cells] + found[:, cells : 2 * cells] + found[:, 2 * cells :]
            return carry

        lax.fori_loop(0, tiles // 2, pair, 0)


def prepare(air_flux, air_area, sea_area, wet, where, tiles, slots, groups=4):
    steps, blocks, fields, cells = air_flux.shape
    return pl.pallas_call(
        prepare_kernel,
        grid=(groups,),
        out_shape=[
            jax.ShapeDtypeStruct((1, cells), jnp.float32),
            jax.ShapeDtypeStruct((slots, cells), jnp.float32),
        ],
        in_specs=[
            pl.BlockSpec((steps, blocks // groups, fields, cells), lambda i: (0, i, 0, 0)),
            pl.BlockSpec((blocks // groups, cells), lambda i: (i, 0)),
            whole(),
            whole(),
            whole(),
            whole(),
        ],
        out_specs=[
            pl.BlockSpec((1, cells), lambda i: (0, 0)),
            pl.BlockSpec((slots, cells), lambda i: (0, 0)),
        ],
        scratch_shapes=[VMEM((fields, cells), jnp.float32)],
        cost_estimate=pl.CostEstimate(
            flops=2 * blocks * slots * tiles.shape[0] * cells * 3,
            bytes_accessed=air_flux.size * 2,
            transcendentals=0,
        ),
        name="prepare",
    )(air_flux, air_area, sea_area, wet, where, tiles)


def partial_kernel(sums_ref, weight_ref, *refs):
    *piece_refs, out_ref = refs
    start = 0
    fields, cells = piece_refs[0].shape[1:]
    sea = jnp.zeros((fields, cells), jnp.float32)
    for piece_ref in piece_refs:
        count = piece_ref.shape[0]
        weight = weight_ref[pl.ds(start, count)]
        sea += jnp.sum(piece_ref[...].astype(jnp.float32) * weight[:, None, :], axis=0)
        start += count
    out_ref[...] = jnp.broadcast_to(sums_ref[...] - lanes_of(sea), out_ref.shape)


def partial(sums, weight, pieces, devices):
    return pl.pallas_call(
        partial_kernel,
        out_shape=jax.ShapeDtypeStruct((devices, sums.shape[1]), jnp.float32),
        in_specs=[whole()] * (2 + len(pieces)),
        out_specs=whole(),
        name="partial",
    )(sums, weight, *pieces)


def regrid_kernel(row_ref, tiles_ref, *refs, group):
    *piece_refs, raw_ref, rows_ref = refs
    start = 0
    for piece_ref in piece_refs:
        count = piece_ref.shape[0]
        rows_ref[start : start + count] = piece_ref[...]
        start += count
    rows_ref[start] = jnp.zeros(rows_ref.shape[1:], rows_ref.dtype)
    tiles, cells, width = tiles_ref.shape
    targets, fields = raw_ref.shape[:2]

    def step(index, carry):
        base = index * group
        total = jnp.zeros((group * fields, width), jnp.float32)
        for tile in range(0, tiles, 2):
            left = jnp.concatenate(
                [
                    jnp.concatenate(
                        [
                            rows_ref[row_ref[(base + target) * tiles + tile + half]]
                            for half in range(2)
                        ],
                        axis=1,
                    )
                    for target in range(group)
                ],
                axis=0,
            )
            right = tiles_ref[tile : tile + 2].reshape(2 * cells, width)
            total += jnp.dot(left, right, preferred_element_type=jnp.float32)
        raw_ref[pl.ds(base, group)] = total.reshape(group, fields, width)
        return carry

    lax.fori_loop(0, targets // group, step, 0)


def regrid(rows, tiles, pieces, targets, group=32):
    fields, cells = pieces[0].shape[1:]
    count = sum(piece.shape[0] for piece in pieces)
    return pl.pallas_call(
        functools.partial(regrid_kernel, group=group),
        out_shape=jax.ShapeDtypeStruct((targets, fields, tiles.shape[2]), jnp.float32),
        in_specs=[whole(SMEM)] + [whole()] * (1 + len(pieces)),
        out_specs=whole(),
        scratch_shapes=[VMEM((count + 1, fields, cells), pieces[0].dtype)],
        cost_estimate=pl.CostEstimate(
            flops=2 * targets * fields * tiles.size, bytes_accessed=tiles.size * 2, transcendentals=0
        ),
        name="regrid",
    )(rows, tiles, *pieces)


def finish_kernel(raw_ref, wet_ref, total_ref, out_ref):
    fields = raw_ref.shape[1]
    cells = raw_ref.shape[2]
    total = jnp.sum(total_ref[...], axis=0, keepdims=True)
    lane = lax.broadcasted_iota(jnp.int32, (fields, cells), 1)
    row = lax.broadcasted_iota(jnp.int32, (fields, cells), 0)
    change = jnp.sum(jnp.where(lane == row, total, 0.0), axis=1, keepdims=True)
    wet = jnp.sum(jnp.where(lane == fields, total, 0.0), axis=1, keepdims=True)
    shift = change / jnp.maximum(wet, 1.0)
    out_ref[...] = wet_ref[...][:, None, :] * (raw_ref[...] + shift[None])


def finish(raw, wet, totals, groups=4):
    targets, fields, cells = raw.shape
    return pl.pallas_call(
        finish_kernel,
        grid=(groups,),
        out_shape=jax.ShapeDtypeStruct(raw.shape, jnp.float32),
        in_specs=[
            pl.BlockSpec((targets // groups, fields, cells), lambda i: (i, 0, 0)),
            pl.BlockSpec((targets // groups, cells), lambda i: (i, 0)),
            whole(),
        ],
        out_specs=pl.BlockSpec((targets // groups, fields, cells), lambda i: (i, 0, 0)),
        name="finish",
    )(raw, wet, totals)


def body(
    air_flux, air_area, sea_area, wet_mask, intersection_tiles, send_block, target_slot, target_tile,
    *, columns, devices,
):
    slots = send_block.shape[1]
    targets = target_slot.shape[0]
    tiles = intersection_tiles.shape[0]
    capacity = slots // columns
    direct = columns & (columns - 1) == 0 and columns <= 8
    order = piece_order(columns) if direct else [0]

    outbound = pick(send_block[0], air_flux, order, "col")
    if direct:
        pieces = [outbound[0]]
        for piece, offset in zip(outbound[1:], order[1:]):
            pairs = [(source, source ^ offset) for source in range(columns)]
            pieces.append(lax.ppermute(piece, "col", pairs))
        me = lax.axis_index("col")
        place = sum(
            jnp.where(target_slot // capacity == me ^ offset, at * capacity, 0)
            for at, offset in enumerate(order)
        )
        slot = place + target_slot % capacity
    else:
        pieces = [lax.all_to_all(outbound[0], "col", split_axis=0, concat_axis=0, tiled=True)]
        slot = target_slot

    match = target_tile[:, :, None] == jnp.arange(tiles, dtype=jnp.int32)[None, None, :]
    rows = slots - jnp.sum(jnp.where(match, slots - slot[:, :, None], 0), axis=1)
    wet = jnp.broadcast_to(wet_mask.astype(jnp.float32)[:, None], sea_area.shape)

    sums, weight = prepare(
        air_flux, air_area, sea_area, wet, rows.T, intersection_tiles, slots
    )
    mine = partial(sums, weight, pieces, devices)
    totals = lax.all_to_all(mine, ("row", "col"), split_axis=0, concat_axis=0, tiled=True)
    raw = regrid(rows.reshape(-1), intersection_tiles, pieces, targets)
    return finish(raw, wet, totals)


def solution(mesh):
    placed = (
        P(None, ("row", "col"), None, None),
        P(("row", "col"), None),
        P(("row", "col"), None),
        P(("row", "col")),
        P(),
        P(("row", "col"), None),
        P(("row", "col"), None),
        P(("row", "col"), None),
    )
    columns = mesh.shape["col"]
    return jax.shard_map(
        functools.partial(body, columns=columns, devices=mesh.shape["row"] * columns),
        mesh=mesh,
        in_specs=placed,
        out_specs=P(("row", "col"), None, None),
        check_vma=False,
    )
```

```python
import functools
import jax
import jax.numpy as jnp
from jax import lax
from jax.experimental import pallas as pl
from jax.experimental.pallas import tpu as pltpu
from jax.sharding import PartitionSpec as P


GROUP = 32
VMEM = pltpu.VMEM
SMEM = pltpu.SMEM


LIMIT = pltpu.CompilerParams(vmem_limit_bytes=12 << 20)


def whole(space=VMEM):
    return pl.BlockSpec(memory_space=space)


def peers_of(columns):
    order = [peer for peer in (2, 4, 3, 5, 6, 7, 1) if peer < columns]
    return order + [peer for peer in range(8, columns)]


def piece_order(columns):
    return [0] + peers_of(columns)


def pick_kernel(send_ref, flux_ref, *refs, order, chunks, axis):
    count = len(order)
    out_refs = refs[:count]
    raw_ref, mean_ref, out_ref, slot_ref, in_sem, slot_sem, out_sem = refs[count:]
    steps, blocks = flux_ref.shape[:2]
    capacity = out_ref.shape[1]
    group = blocks // chunks
    fetches = []
    for chunk in range(chunks):
        part = pl.ds(chunk * group, group)
        fetches.append(
            pltpu.make_async_copy(flux_ref.at[:, part], raw_ref.at[:, part], in_sem.at[chunk])
        )
        fetches[-1].start()
    fetch_slots = pltpu.make_async_copy(send_ref, slot_ref, slot_sem)
    fetch_slots.start()
    for chunk in range(chunks):
        part = pl.ds(chunk * group, group)
        fetches[chunk].wait()
        total = raw_ref[0, part].astype(jnp.float32)
        for step in range(1, steps):
            total += raw_ref[step, part].astype(jnp.float32)
        mean_ref[part] = (total * (1.0 / steps)).astype(mean_ref.dtype)
    fetch_slots.wait()
    me = lax.axis_index(axis) if count > 1 else 0
    stores = []
    for index, offset in enumerate(order):
        base = (me ^ offset) * capacity
        for slot in range(capacity):
            out_ref[index, slot] = mean_ref[slot_ref[0, base + slot]]
        stores.append(
            pltpu.make_async_copy(out_ref.at[index], out_refs[index], out_sem.at[index])
        )
        stores[-1].start()
    for store in stores:
        store.wait()


def pick(send_block, air_flux, order, axis, chunks=8):
    steps, blocks, fields, cells = air_flux.shape
    count = len(order)
    capacity = send_block.shape[1] // count
    dtype = air_flux.dtype
    return pl.pallas_call(
        functools.partial(pick_kernel, order=order, chunks=chunks, axis=axis),
        out_shape=[jax.ShapeDtypeStruct((capacity, fields, cells), dtype)] * count,
        in_specs=[whole(pl.ANY)] * 2,
        out_specs=[whole(pl.ANY)] * count,
        scratch_shapes=[
            VMEM(air_flux.shape, dtype),
            VMEM((blocks, fields, cells), dtype),
            VMEM((count, capacity, fields, cells), dtype),
            SMEM(send_block.shape, send_block.dtype),
            pltpu.SemaphoreType.DMA((chunks,)),
            pltpu.SemaphoreType.DMA,
            pltpu.SemaphoreType.DMA((count,)),
        ],
        name="pick",
    )(send_block, air_flux)


def air_kernel(flux_ref, area_ref, air_ref):
    steps, blocks = flux_ref.shape[:2]
    air = [jnp.zeros(air_ref.shape, jnp.float32)] * 4
    for block in range(blocks):
        total = flux_ref[0, block].astype(jnp.float32)
        for step in range(1, steps):
            total += flux_ref[step, block].astype(jnp.float32)
        air[block % 4] += (total * (1.0 / steps)) * area_ref[block : block + 1, :]
    air_ref[...] = (air[0] + air[1]) + (air[2] + air[3])


def air_sums(flux, area):
    return pl.pallas_call(
        air_kernel,
        out_shape=jax.ShapeDtypeStruct(flux.shape[2:], jnp.float32),
        in_specs=[whole()] * 2,
        out_specs=whole(),
        cost_estimate=pl.CostEstimate(
            flops=8 * flux.size, bytes_accessed=2 * flux.size, transcendentals=0
        ),
        compiler_params=LIMIT,
        name="air",
    )(flux, area)


def split(value):
    high = value.astype(jnp.bfloat16)
    return high, (value - high.astype(jnp.float32)).astype(jnp.bfloat16)


def lanes_of(column):
    rows, lanes = column.shape
    total = jnp.sum(column, axis=1, keepdims=True)
    on = lax.broadcasted_iota(jnp.int32, (rows, lanes), 0) == lax.broadcasted_iota(
        jnp.int32, (rows, lanes), 1
    )
    return jnp.sum(jnp.where(on, total, 0.0), axis=0, keepdims=True)


def prepare_kernel(
    air_ref, sea_ref, wet_ref, where_ref, tiles_ref, own_ref, list_ref, sums_ref, weight_ref, kept_ref, listed_ref
):
    fields, cells = air_ref.shape
    kept_ref[...] = own_ref[...]
    listed_ref[...] = list_ref[...]
    wet_area = wet_ref[...] * sea_ref[...]
    wet_row = jnp.sum(jnp.sum(wet_area, axis=0, keepdims=True), axis=1, keepdims=True)
    lane = lax.broadcasted_iota(jnp.int32, (1, cells), 1)
    parts = jnp.concatenate(split(wet_area), axis=0)
    targets = wet_area.shape[0]
    slots = weight_ref.shape[0]
    tiles = where_ref.shape[0]
    slot = lax.broadcasted_iota(jnp.int32, (slots, targets), 0)
    weight = jnp.zeros((slots, 2 * cells), jnp.float32)
    for tile in range(0, tiles, 2):
        spread = lax.dot_general(
            parts,
            tiles_ref[tile : tile + 2].reshape(2 * cells, cells),
            (((1,), (1,)), ((), ())),
            preferred_element_type=jnp.float32,
        )
        spread = spread[:targets] + spread[targets:]
        values = [
            jnp.concatenate(split(spread[:, half * cells : (half + 1) * cells]), axis=1)
            for half in range(2)
        ]
        hits = [
            jnp.where(slot == where_ref[pl.ds(tile + half, 1), :], 1.0, 0.0).astype(jnp.bfloat16)
            for half in range(2)
        ]
        weight += jnp.dot(
            jnp.concatenate(hits, axis=1),
            jnp.concatenate(values, axis=0),
            preferred_element_type=jnp.float32,
        )
    weight = weight[:, :cells] + weight[:, cells:]
    weight_ref[...] = weight
    seas = [air_ref[...]] + [jnp.zeros((fields, cells), jnp.float32)] * 3
    if own_ref.shape[0] < weight_ref.shape[0]:
        for row in range(own_ref.shape[0]):
            seas[row % 4] -= own_ref[row].astype(jnp.float32) * weight_ref[row : row + 1, :]
    sums = lanes_of((seas[0] + seas[1]) + (seas[2] + seas[3]))
    sums_ref[...] = sums + jnp.where(lane == fields, wet_row, 0.0)


def prepare(air, sea_area, wet, where, tiles, own, listed, slots):
    fields, cells = air.shape
    return pl.pallas_call(
        prepare_kernel,
        out_shape=[
            jax.ShapeDtypeStruct((1, cells), jnp.float32),
            jax.ShapeDtypeStruct((slots, cells), jnp.float32),
            jax.ShapeDtypeStruct(own.shape, own.dtype),
            jax.ShapeDtypeStruct(listed.shape, listed.dtype),
        ],
        in_specs=[whole()] * 7,
        out_specs=[whole()] * 4,
        cost_estimate=pl.CostEstimate(
            flops=2 * wet.shape[0] * slots * tiles.shape[0] * cells * 3,
            bytes_accessed=tiles.size * 2,
            transcendentals=0,
        ),
        compiler_params=LIMIT,
        name="prepare",
    )(air, sea_area, wet, where, tiles, own, listed)


def partial_kernel(sums_ref, weight_ref, *refs):
    *piece_refs, out_ref = refs
    fields, cells = piece_refs[0].shape[1:]
    start = weight_ref.shape[0] - sum(piece_ref.shape[0] for piece_ref in piece_refs)
    seas = [jnp.zeros((fields, cells), jnp.float32)] * 4
    for piece_ref in piece_refs:
        count = piece_ref.shape[0]
        for row in range(count):
            weight = weight_ref[start + row : start + row + 1, :]
            seas[row % 4] += piece_ref[row].astype(jnp.float32) * weight
        start += count
    sea = (seas[0] + seas[1]) + (seas[2] + seas[3])
    out_ref[...] = jnp.broadcast_to(sums_ref[...] - lanes_of(sea), out_ref.shape)


def partial(sums, weight, pieces, devices):
    return pl.pallas_call(
        partial_kernel,
        out_shape=jax.ShapeDtypeStruct((devices, sums.shape[1]), jnp.float32),
        in_specs=[whole()] * (2 + len(pieces)),
        out_specs=whole(),
        compiler_params=LIMIT,
        name="partial",
    )(sums, weight, *pieces)


def regrid_kernel(where_ref, tiles_ref, *refs, group):
    *piece_refs, raw_ref, rows_ref, row_ref, row_sem = refs
    fetch = pltpu.make_async_copy(where_ref, row_ref, row_sem)
    fetch.start()
    start = 0
    for piece_ref in piece_refs:
        count = piece_ref.shape[0]
        rows_ref[start : start + count] = piece_ref[...]
        start += count
    rows_ref[start] = jnp.zeros(rows_ref.shape[1:], rows_ref.dtype)
    tiles, cells, width = tiles_ref.shape
    targets, fields = raw_ref.shape[:2]
    fetch.wait()

    def step(index, carry):
        base = index * group
        total = jnp.zeros((group * fields, width), jnp.float32)
        for tile in range(0, tiles, 2):
            left = jnp.concatenate(
                [
                    jnp.concatenate(
                        [
                            rows_ref[row_ref[(base + target) * tiles + tile + half]]
                            for half in range(2)
                        ],
                        axis=1,
                    )
                    for target in range(group)
                ],
                axis=0,
            )
            right = tiles_ref[tile : tile + 2].reshape(2 * cells, width)
            total += jnp.dot(left, right, preferred_element_type=jnp.float32)
        raw_ref[pl.ds(base, group)] = total.reshape(group, fields, width)
        return carry

    lax.fori_loop(0, targets // group, step, 0)


def regrid(where, tiles, pieces, targets, group=GROUP):
    fields, cells = pieces[0].shape[1:]
    count = sum(piece.shape[0] for piece in pieces)
    return pl.pallas_call(
        functools.partial(regrid_kernel, group=group),
        out_shape=jax.ShapeDtypeStruct((targets, fields, tiles.shape[2]), jnp.float32),
        in_specs=[whole(pl.ANY)] + [whole()] * (1 + len(pieces)),
        out_specs=whole(),
        scratch_shapes=[
            VMEM((count + 1, fields, cells), pieces[0].dtype),
            SMEM(where.shape, where.dtype),
            pltpu.SemaphoreType.DMA,
        ],
        cost_estimate=pl.CostEstimate(
            flops=2 * targets * fields * tiles.size, bytes_accessed=tiles.size * 2, transcendentals=0
        ),
        compiler_params=LIMIT,
        name="regrid",
    )(where, tiles, *pieces)


def finish_kernel(raw_ref, wet_ref, total_ref, out_ref):
    fields = raw_ref.shape[1]
    cells = raw_ref.shape[2]
    total = jnp.sum(total_ref[...], axis=0, keepdims=True)
    lane = lax.broadcasted_iota(jnp.int32, (fields, cells), 1)
    row = lax.broadcasted_iota(jnp.int32, (fields, cells), 0)
    change = jnp.sum(jnp.where(lane == row, total, 0.0), axis=1, keepdims=True)
    wet = jnp.sum(jnp.where(lane == fields, total, 0.0), axis=1, keepdims=True)
    shift = change / jnp.maximum(wet, 1.0)
    out_ref[...] = wet_ref[...][:, None, :] * (raw_ref[...] + shift[None])


def finish(raw, wet, totals, groups=2):
    targets, fields, cells = raw.shape
    return pl.pallas_call(
        finish_kernel,
        grid=(groups,),
        out_shape=jax.ShapeDtypeStruct(raw.shape, jnp.float32),
        in_specs=[
            pl.BlockSpec((targets // groups, fields, cells), lambda i: (i, 0, 0)),
            pl.BlockSpec((targets // groups, cells), lambda i: (i, 0)),
            whole(),
        ],
        out_specs=pl.BlockSpec((targets // groups, fields, cells), lambda i: (i, 0, 0)),
        compiler_params=LIMIT,
        name="finish",
    )(raw, wet, totals)


def body(
    air_flux, air_area, sea_area, wet_mask, intersection_tiles, send_block, target_slot, target_tile,
    *, columns, devices,
):
    slots = send_block.shape[1]
    targets = target_slot.shape[0]
    tiles = intersection_tiles.shape[0]
    capacity = slots // columns
    direct = columns & (columns - 1) == 0 and columns <= 8
    order = piece_order(columns) if direct else [0]

    outbound = pick(send_block, air_flux, order, "col")
    if direct:
        pieces = [outbound[0]]
        for piece, offset in zip(outbound[1:], order[1:]):
            pairs = [(source, source ^ offset) for source in range(columns)]
            pieces.append(lax.ppermute(piece, "col", pairs))
        me = lax.axis_index("col")
        place = sum(
            jnp.where(target_slot // capacity == me ^ offset, at * capacity, 0)
            for at, offset in enumerate(order)
        )
        slot = place + target_slot % capacity
    else:
        pieces = [lax.all_to_all(outbound[0], "col", split_axis=0, concat_axis=0, tiled=True)]
        slot = target_slot

    match = target_tile[:, :, None] == jnp.arange(tiles, dtype=jnp.int32)[None, None, :]
    rows = slots - jnp.sum(jnp.where(match, slots - slot[:, :, None], 0), axis=1)
    wet = jnp.broadcast_to(wet_mask.astype(jnp.float32)[:, None], sea_area.shape)

    own = pieces[0]
    sums, weight, kept, listed = prepare(
        air_sums(air_flux, air_area), sea_area, wet, rows.T, intersection_tiles, own, rows.reshape(-1), slots
    )
    received = pieces[1:] if direct else pieces
    mine = partial(sums, weight, received, devices)
    totals = lax.all_to_all(mine, ("row", "col"), split_axis=0, concat_axis=0, tiled=True)
    raw = regrid(listed, intersection_tiles, [kept, *received] if direct else received, targets)
    return finish(raw, wet, totals)


def solution(mesh):
    placed = (
        P(None, ("row", "col"), None, None),
        P(("row", "col"), None),
        P(("row", "col"), None),
        P(("row", "col")),
        P(),
        P(("row", "col"), None),
        P(("row", "col"), None),
        P(("row", "col"), None),
    )
    columns = mesh.shape["col"]
    return jax.shard_map(
        functools.partial(body, columns=columns, devices=mesh.shape["row"] * columns),
        mesh=mesh,
        in_specs=placed,
        out_specs=P(("row", "col"), None, None),
        check_vma=False,
    )
```
